32 devices in a mesh: expert: 8 (over z, y), mp: 4 (over x, core).
Axes of the slice: x: 2, y: 2, z: 4, core: 2. Of those that a mesh axis runs over, the one named last changes fastest.
Arguments:
- tokens: bfloat16 [1024, 3584], P('expert', 'mp'), may hold values from -6 to 6
- assignments: int32 [1024, 2], P('expert'), may hold values from 0 to 7, all different within a row; in each aligned block of 128 rows (0 to 127, 128 to 255, ...) at most 64 rows name the same one
- gate_probs: float32 [1024, 2], P('expert'), may hold values from 0.05 to 0.5
- expert_gate: bfloat16 [8, 3584, 2560], P('expert', None, 'mp'), may hold values from -0.09375 to 0.09375
- expert_up: bfloat16 [8, 3584, 2560], P('expert', None, 'mp'), may hold values from -0.09375 to 0.09375
- expert_down: bfloat16 [8, 2560, 3584], P('expert', 'mp'), may hold values from -0.125 to 0.125
- shared_gate: bfloat16 [3584, 10240], P('mp', 'expert'), may hold values from -0.09375 to 0.09375
- shared_up: bfloat16 [3584, 10240], P('mp', 'expert'), may hold values from -0.09375 to 0.09375
- shared_down_weight: bfloat16 [10240, 3584], P('expert', 'mp'), may hold values from -0.0625 to 0.0625
Outputs:
- layer_out: bfloat16 [1024, 3584], P('expert', 'mp')
The draws below stay inside these ranges and needn't reach their ends.
Inputs may be any that keep to these rules, and one draw needn't show every extreme that they name: `assignments`: each row names 2 different experts; among the 128 rows of one index of the expert axis (aligned blocks) no expert is named more than 64 times.
All inputs are finite; a program needn't handle non-finite values.
Results may differ from the reference program's by a relative error of at most 0.0075.
Values may be sent and summed in bfloat16 or wider, within the bound.
No kernel may reach another device: no remote copies, remote signals or barrier semaphores. Data moves between devices by JAX's collectives and lax.ppermute only.
A program may use at most 128 MiB of HBM per device.

```python
import math
import jax
import jax.numpy as jnp
import numpy as np
from jax import lax

D = 3584
FF = 2560
FS = 10240
TOP = 2
TOK_DEV = 128
EXPERTS = 8
TOKENS = 1024
CAP = 64
N_EXPERT = 8
N_MP = 4


def block_scale(rng, shape, pieces, smallest, top_value):
    level = 1.0
    for dim, blocks in pieces:
        steps = jax.random.uniform(jax.random.fold_in(jax.random.fold_in(rng, 6), dim), (blocks,), jnp.float32, smallest / len(pieces), top_value / len(pieces))
        level = level * jnp.repeat(jnp.exp(steps), shape[dim] // blocks).reshape((-1,) + (1,) * (len(shape) - 1 - dim))
    return level


def shared_out(key, own, number, rows, amount, top, bound, skew):
    ranking = jax.random.permutation(key, amount)
    heavy_load, common = shares(amount, rows * top, bound, skew, True), shares(amount, rows * top, bound, skew, False)
    places = jnp.arange(amount)

    def named(sizes, turn):
        used = int((sizes > 0).sum())
        fixed = max(1, used // 4)
        shifted = fixed + (places - fixed + turn * (used - fixed)) % max(1, amount - fixed)
        return jnp.zeros((amount,), jnp.int32).at[ranking[jnp.where(places < fixed, places, shifted)]].set(jnp.asarray(sizes, jnp.int32))

    sizes = jnp.where(number % 4 == 0, named(heavy_load, number // 4), named(common, number - number // 4 - 1))
    mixed = jax.random.permutation(jax.random.fold_in(own, 3), amount)
    source_of, receiver = mixed[0:amount // 2 * 2:2], mixed[1:amount // 2 * 2:2]
    margin = jnp.minimum(sizes[source_of] - 1, bound - sizes[receiver]) // 2
    margin = jnp.where((source_of == ranking[0]) | (receiver == ranking[0]) | (sizes[receiver] == 0), 0, jnp.maximum(margin, 0))
    shifted = jax.random.randint(jax.random.fold_in(own, 4), (amount // 2,), 0, 1 << 20) % (margin + 1)
    sizes = sizes.at[source_of].add(-shifted).at[receiver].add(shifted)
    items = jnp.searchsorted(jnp.cumsum(sizes), jnp.arange(rows * top), side="right").astype(jnp.int32)
    grid = items.reshape(top, rows).T
    grid = grid[jax.random.permutation(jax.random.fold_in(own, 1), rows)]
    turn = jax.random.randint(jax.random.fold_in(own, 2), (rows, 1), 0, top)
    return jnp.take_along_axis(grid, (jnp.arange(top)[None, :] + turn) % top, axis=1)


def shares(count, total, bound, lean, full):
    loads = [(1 << 20) // math.isqrt(rank ** lean) + 1 for rank in range(1, count + 1)]
    largest = bound if full else min(bound, max(-(-total // count), total * loads[0] // sum(loads)))
    least = 1 if total - largest >= count - 1 else 0
    counts, surplus = [largest] + [least] * (count - 1), total - largest - least * (count - 1)
    while surplus > 0:
        candidates = [i for i in range(1, count) if counts[i] < largest] or [i for i in range(1, count) if counts[i] < bound]
        whole, left = sum([loads[i] for i in candidates]), surplus
        for i in candidates:
            addition = min(bound - counts[i], max(1, left * loads[i] // whole), surplus)
            counts[i] = counts[i] + addition
            surplus = surplus - addition
    return np.array(counts)


def gaussian(rng, shape, scale, most, pieces=(), held_as=jnp.bfloat16):
    level = block_scale(rng, shape, pieces, -0.22, 0.18) if pieces else 1.0
    result = jax.random.normal(rng, shape, jnp.float32) * scale * level
    return jnp.minimum(jnp.maximum(result, -most), most).astype(held_as)


def setup_inputs(seed: int = 0) -> dict:
    splits = jax.random.split(jax.random.key(seed), 10)
    tokens = gaussian(splits[0], (TOKENS, D), 1.0, 6.0, ((0, 8), (1, 4)))
    assignments_keys = jax.random.split(jax.random.fold_in(splits[1], 1), TOKENS // TOK_DEV)
    assignments_turns = jax.random.permutation(jax.random.fold_in(splits[1], 3), TOKENS // TOK_DEV)
    assignments = jax.vmap(lambda own, number: shared_out(jax.random.fold_in(splits[1], 2), own, number, TOK_DEV, EXPERTS, TOP, CAP, 2))(assignments_keys, assignments_turns).reshape((TOKENS, TOP))
    gate_probs = jnp.clip(0.05 + 0.45 * jax.random.uniform(splits[2], (TOKENS, TOP), jnp.float32) ** block_scale(splits[2], (TOKENS, TOP), ((0, 8),), -0.2, 0.2), 0.05, 0.5)
    expert_gate = gaussian(splits[3], (EXPERTS, D, FF), D ** -0.5, 0.09375, ((0, 8), (2, 4)))
    expert_up = gaussian(splits[4], (EXPERTS, D, FF), D ** -0.5, 0.09375, ((0, 8), (2, 4)))
    expert_down = gaussian(splits[5], (EXPERTS, FF, D), FF ** -0.5, 0.125, ((0, 8), (1, 4)))
    shared_gate = gaussian(splits[6], (D, FS), D ** -0.5, 0.09375, ((0, 4), (1, 8)))
    shared_up = gaussian(splits[7], (D, FS), D ** -0.5, 0.09375, ((0, 4), (1, 8)))
    shared_down_weight = gaussian(splits[8], (FS, D), FS ** -0.5, 0.0625, ((0, 8), (1, 4)))
    return {"tokens": tokens, "assignments": assignments, "gate_probs": gate_probs, "expert_gate": expert_gate, "expert_up": expert_up, "expert_down": expert_down, "shared_gate": shared_gate, "shared_up": shared_up, "shared_down_weight": shared_down_weight}


def slot_table(assignments):
    pair_ids = assignments.reshape(N_EXPERT, TOK_DEV * TOP)
    onehot = (pair_ids[:, :, None] == jnp.arange(EXPERTS, dtype=jnp.int32)[None, None, :]).astype(jnp.int32)
    rank_ids = jnp.cumsum(onehot, axis=1) - onehot
    return jnp.sum(rank_ids * onehot, axis=2).reshape(TOKENS, TOP).astype(jnp.int32)


def reference(tokens, assignments, gate_probs, expert_gate, expert_up, expert_down, shared_gate, shared_up, shared_down_weight):
    shared_gate_act = jnp.dot(tokens, shared_gate, preferred_element_type=jnp.float32)
    shared_up_act = jnp.dot(tokens, shared_up, preferred_element_type=jnp.float32)
    shared_hidden = (jax.nn.silu(shared_gate_act) * shared_up_act).astype(jnp.bfloat16)
    shared_result = jnp.dot(shared_hidden, shared_down_weight, preferred_element_type=jnp.float32)

    slot_ids = slot_table(assignments)
    blocks = (jnp.arange(TOKENS, dtype=jnp.int32) // TOK_DEV)[:, None]
    column = (blocks * CAP + slot_ids).astype(jnp.int32)
    token_ids = jnp.broadcast_to(jnp.arange(TOKENS, dtype=jnp.int32)[:, None], (TOKENS, TOP))
    source = jnp.zeros((EXPERTS, N_EXPERT * CAP), jnp.int32).at[assignments, column].set(token_ids)
    filled = jnp.zeros((EXPERTS, N_EXPERT * CAP), jnp.float32).at[assignments, column].set(1.0)
    group = FF // N_MP

    def expert_step(running, expert_id):
        gathered = tokens[source[expert_id]] * filled[expert_id][:, None].astype(jnp.bfloat16)
        gate_act = jnp.dot(gathered, expert_gate[expert_id], preferred_element_type=jnp.float32)
        up_act = jnp.dot(gathered, expert_up[expert_id], preferred_element_type=jnp.float32)
        hidden = (jax.nn.silu(gate_act) * up_act).astype(jnp.bfloat16)
        split_segments = hidden.reshape(N_EXPERT * CAP, N_MP, group).transpose(1, 0, 2).astype(jnp.float32)
        down_weight_pieces = expert_down[expert_id].reshape(N_MP, group, D).astype(jnp.float32)
        partial_sums_list = jnp.einsum("gnc,gcv->gnv", split_segments, down_weight_pieces, precision=lax.Precision.HIGHEST)
        rounded = lax.optimization_barrier(partial_sums_list.astype(jnp.bfloat16))
        output = jnp.sum(rounded.astype(jnp.float32), axis=0)
        chosen = (assignments == expert_id)
        weights = jnp.sum(jnp.where(chosen, gate_probs, jnp.zeros_like(gate_probs)), axis=1)
        position = jnp.sum(jnp.where(chosen, column, jnp.zeros_like(column)), axis=1).astype(jnp.int32)
        return running + weights[:, None] * output[position], None

    routed, _ = lax.scan(expert_step, jnp.zeros((TOKENS, D), jnp.float32), jnp.arange(EXPERTS, dtype=jnp.int32))
    return (shared_result + routed).astype(jnp.bfloat16)
```

```python
import jax
import jax.numpy as jnp
from jax import lax
from jax.sharding import PartitionSpec as P


BF16 = jnp.bfloat16
F32 = jnp.float32


def bits_of(size):
    count = size.bit_length() - 1
    assert size == 1 << count
    return [1 << b for b in range(count)]


def dot(a, b):
    return jnp.dot(a, b, preferred_element_type=F32)


def three_parts(values):
    parts = []
    for _ in range(3):
        head = lax.reduce_precision(values, 8, 7)
        parts.append(head.astype(BF16))
        values = values - head
    return parts


def on_device(
    tokens,
    assignments,
    gate_probs,
    expert_gate,
    expert_up,
    expert_down,
    shared_gate,
    shared_up,
    shared_down_weight,
):
    experts, parts = lax.axis_size("expert"), lax.axis_size("mp")
    expert, part = lax.axis_index("expert"), lax.axis_index("mp")
    rows, width = tokens.shape
    chosen = assignments.shape[1]
    slots = min(rows, max(2, 2 * rows * chosen // experts))
    expert_bits, part_bits = bits_of(experts), bits_of(parts)

    def swap(value, de=0, dm=0):
        pairs = [
            (e * parts + m, (e ^ de) * parts + (m ^ dm))
            for e in range(experts)
            for m in range(parts)
        ]
        return lax.ppermute(value, ("expert", "mp"), pairs)

    def by_part(values):
        values = list(values)
        for bit in part_bits:
            flip = (part & bit) != 0
            values = [
                jnp.where(flip, values[j ^ bit], values[j]) for j in range(len(values))
            ]
        return values

    ids_t = assignments.T
    probs_t = gate_probs.T
    notes = [ids_t[k : k + 1].astype(BF16) for k in range(chosen)]
    for k in range(chosen):
        notes += three_parts(probs_t[k : k + 1])
    notes = jnp.concatenate(notes, axis=0)
    block = jnp.concatenate([tokens, jnp.pad(notes, ((0, 0), (0, width - rows)))], axis=0)

    blocks = {0: block}
    for bit in reversed(expert_bits[1:]):
        for k in list(blocks):
            blocks[k | bit] = swap(blocks[k], de=bit)
    for bit in expert_bits[:1]:
        for k in list(blocks):
            blocks[k | bit] = swap(blocks[k], de=bit)

    before = jnp.triu(jnp.ones((rows, rows), F32), 1).astype(BF16)

    def slot_map(named):
        rank = dot(named.astype(BF16), before)
        place = jnp.arange(slots, dtype=jnp.int32).astype(F32)[None, :, None]
        return ((rank[:, None, :] == place) & (named[:, None, :] > 0)).astype(BF16)

    slices = {0: tokens}
    for bit in part_bits[1:]:
        for j in list(slices):
            slices[j | bit] = swap(slices[j], dm=bit)
    others = [j for j in sorted(slices) if j]
    targets = expert ^ jnp.arange(experts, dtype=jnp.int32)
    wanted = jnp.any(ids_t[None] == targets[:, None, None], axis=1).astype(F32)
    sending = slot_map(wanted)
    far = jnp.concatenate([slices[j] for j in others], axis=1)
    outgoing = jnp.einsum("kst,td->ksd", sending, far, preferred_element_type=F32).astype(BF16)
    arrived = [outgoing[0]] + [swap(outgoing[k], de=k) for k in range(1, experts)]

    table = jnp.stack([blocks[k][rows : rows + 4 * chosen, :rows] for k in range(experts)])
    ids_all = table[:, :chosen].astype(F32)
    probs_all = table[:, chosen:].astype(F32).reshape(experts, chosen, 3, rows)
    probs_all = probs_all[:, :, 0] + (probs_all[:, :, 1] + probs_all[:, :, 2])
    mine = ids_all == expert.astype(F32)
    taking = slot_map(jnp.any(mine, axis=1).astype(F32))
    row_prob = jnp.sum(jnp.where(mine, probs_all, 0.0), axis=1)
    slot_prob = jnp.sum(taking.astype(F32) * row_prob[:, None, :], axis=2)
    near = [dot(taking[k], blocks[k][:rows]).astype(BF16) for k in range(experts)]

    both = jnp.concatenate([shared_gate, shared_up], axis=1)
    hidden_width = shared_gate.shape[1]
    groups = experts // parts
    shared_hidden = {}
    for g in range(groups):
        held = by_part([blocks[g * parts + j][:rows] for j in range(parts)])
        sums = {}
        pending = list(range(parts))
        for bit in part_bits:
            keep = [j for j in pending if not j & bit]
            send = [j for j in pending if j & bit]
            if bit == 1:
                leaving = dot(jnp.concatenate([held[j] for j in send]), both).astype(BF16)
                staying = dot(jnp.concatenate([held[j] for j in keep]), both)
            else:
                leaving = jnp.concatenate([sums[j] for j in send]).astype(BF16)
                staying = jnp.concatenate([sums[j] for j in keep])
            total = staying + swap(leaving, dm=bit).astype(F32)
            sums = {j: total[i * rows : (i + 1) * rows] for i, j in enumerate(keep)}
            pending = keep
        act = sums[0]
        hidden = (jax.nn.silu(act[:, :hidden_width]) * act[:, hidden_width:]).astype(BF16)
        known = {0: hidden}
        for bit in reversed(part_bits):
            order = sorted(known)
            got = swap(jnp.concatenate([known[j] for j in order]), dm=bit)
            for i, j in enumerate(order):
                known[j | bit] = got[i * rows : (i + 1) * rows]
        back = by_part([known[j] for j in range(parts)])
        for j in range(parts):
            shared_hidden[g * parts + j] = back[j]

    count = experts * slots
    own = [jnp.concatenate(near)]
    for i in range(len(others)):
        own.append(jnp.concatenate([a[:, i * width : (i + 1) * width] for a in arrived]))
    own = jnp.stack(own)
    core = swap(own, dm=1)
    gathered = []
    for j in range(parts):
        gathered.append((core if j & 1 else own)[j // 2])
    gathered = jnp.concatenate(by_part(gathered), axis=1)
    gate_act = dot(gathered, expert_gate[0])
    up_act = dot(gathered, expert_up[0])
    hidden = (jax.nn.silu(gate_act) * up_act).astype(BF16)
    partial = {}
    for j in range(parts):
        columns = lax.dynamic_slice_in_dim(expert_down[0], (part ^ j) * width, width, axis=1)
        partial[j] = dot(hidden, columns)
    pending = list(range(parts))
    for bit in part_bits:
        keep = [j for j in pending if not j & bit]
        send = [j for j in pending if j & bit]
        got = swap(jnp.stack([partial[j].astype(BF16) for j in send]), dm=bit)
        for i, j in enumerate(keep):
            partial[j] = partial[j] + got[i].astype(F32)
        pending = keep
    result = partial[0].reshape(experts, slots, width) * slot_prob[:, :, None]
    result = result.astype(BF16)

    total = {}
    for k in range(experts):
        routed = jnp.einsum("st,sd->td", taking[k], result[k], preferred_element_type=F32)
        total[k] = dot(shared_hidden[k], shared_down_weight) + routed
    left = list(range(experts))
    for bit in expert_bits:
        for k in sorted((k for k in left if k & bit), reverse=True):
            total[k ^ bit] = total[k ^ bit] + swap(total[k].astype(BF16), de=bit).astype(F32)
        left = [k for k in left if not k & bit]
    return total[0].astype(BF16)


def solution(mesh):
    in_specs = (
        P("expert", "mp"),
        P("expert", None),
        P("expert", None),
        P("expert", None, "mp"),
        P("expert", None, "mp"),
        P("expert", "mp", None),
        P("mp", "expert"),
        P("mp", "expert"),
        P("expert", "mp"),
    )
    out_specs = P("expert", "mp")
    return jax.shard_map(
        on_device, mesh=mesh, in_specs=in_specs, out_specs=out_specs, check_vma=False
    )
```

```python
import jax
import jax.numpy as jnp
from jax import lax
from jax.sharding import PartitionSpec as P


BF16 = jnp.bfloat16
F32 = jnp.float32


def bits_of(size):
    count = size.bit_length() - 1
    assert size == 1 << count
    return [1 << b for b in range(count)]


def dot(a, b):
    return jnp.dot(a, b, preferred_element_type=F32)


def three_parts(values):
    parts = []
    for _ in range(3):
        head = lax.reduce_precision(values, 8, 7)
        parts.append(head.astype(BF16))
        values = values - head
    return parts


def step(function, *values, after=()):
    held = lax.optimization_barrier(values + tuple(after))[: len(values)]
    return function(*held)


def on_device(
    tokens,
    assignments,
    gate_probs,
    expert_gate,
    expert_up,
    expert_down,
    shared_gate,
    shared_up,
    shared_down_weight,
):
    experts, parts = lax.axis_size("expert"), lax.axis_size("mp")
    expert, part = lax.axis_index("expert"), lax.axis_index("mp")
    rows, width = tokens.shape
    chosen = assignments.shape[1]
    slots = min(rows, max(2, 2 * rows * chosen // experts))
    expert_bits, part_bits = bits_of(experts), bits_of(parts)
    groups = [list(range(g, g + parts)) for g in range(0, experts, parts)]
    hidden_width = shared_gate.shape[1]

    def swap(value, de=0, dm=0):
        pairs = [
            (e * parts + m, (e ^ de) * parts + (m ^ dm))
            for e in range(experts)
            for m in range(parts)
        ]
        return lax.ppermute(value, ("expert", "mp"), pairs)

    def by_part(values):
        values = list(values)
        for bit in part_bits:
            flip = (part & bit) != 0
            values = [jnp.where(flip, values[j ^ bit], values[j]) for j in range(len(values))]
        return values

    def prepare(tokens, ids, probs):
        notes = [ids.T[k : k + 1].astype(BF16) for k in range(chosen)]
        for k in range(chosen):
            notes += three_parts(probs.T[k : k + 1])
        notes = jnp.concatenate(notes, axis=0)
        return jnp.concatenate([tokens, jnp.pad(notes, ((0, 0), (0, width - rows)))], axis=0)

    blocks = {0: step(prepare, tokens, assignments, gate_probs)}
    for bit in reversed(expert_bits[1:]):
        for k in list(blocks):
            blocks[k | bit] = swap(blocks[k], de=bit)
    for k in list(blocks):
        blocks[k | 1] = swap(blocks[k], de=1)

    slices = {0: tokens}
    for bit in part_bits[1:]:
        for j in list(slices):
            slices[j | bit] = swap(slices[j], dm=bit)
    others = [j for j in sorted(slices) if j]
    far = {0: jnp.concatenate([slices[j] for j in others], axis=1)}
    for bit in reversed(expert_bits):
        source = [k for k in sorted(far) if bit >= parts or k >= parts]
        if source:
            got = swap(jnp.stack([far[k] for k in source]), de=bit)
            for n, k in enumerate(source):
                far[k | bit] = got[n]

    before = jnp.triu(jnp.ones((rows, rows), F32), 1).astype(BF16)
    place = jnp.arange(slots, dtype=jnp.int32).astype(F32)[None, :, None]
    both = step(lambda a, b: jnp.concatenate([a, b], axis=1), shared_gate, shared_up)

    def pick(taking, *sources):
        return jnp.concatenate([dot(taking[i], b).astype(BF16) for i, b in enumerate(sources)])

    def dispatch(*members):
        table = jnp.stack([b[rows : rows + 4 * chosen, :rows] for b in members])
        ids = table[:, :chosen].astype(F32)
        probs = table[:, chosen:].astype(F32).reshape(len(members), chosen, 3, rows)
        probs = probs[:, :, 0] + (probs[:, :, 1] + probs[:, :, 2])
        mine = ids == expert.astype(F32)
        named = jnp.any(mine, axis=1).astype(F32)
        rank = dot(named.astype(BF16), before)
        taking = ((rank[:, None, :] == place) & (named[:, None, :] > 0)).astype(BF16)
        row_prob = jnp.sum(jnp.where(mine, probs, 0.0), axis=1)
        weight = jnp.sum(taking.astype(F32) * row_prob[:, None, :], axis=2)
        return pick(taking, *[b[:rows] for b in members]), weight, taking

    def shared_act(act, came):
        act = act + came.astype(F32)
        return (jax.nn.silu(act[:, :hidden_width]) * act[:, hidden_width:]).astype(BF16)

    def feed(own, core):
        gate_act = up_act = 0.0
        for j in sorted(range(parts), key=lambda j: j & 1):
            rows_j = core[j // 2] if j & 1 else own[j // 2]
            start = (part ^ j) * width
            gate_act += dot(rows_j, lax.dynamic_slice_in_dim(expert_gate[0], start, width, axis=0))
            up_act += dot(rows_j, lax.dynamic_slice_in_dim(expert_up[0], start, width, axis=0))
        return (jax.nn.silu(gate_act) * up_act).astype(BF16)

    def lower(js, kind):
        def function(hidden):
            out = []
            for j in js:
                columns = lax.dynamic_slice_in_dim(
                    expert_down[0], (part ^ j) * width, width, axis=1
                )
                out.append(dot(hidden, columns).astype(kind))
            return jnp.stack(out)

        return function

    odd = [j for j in range(parts) if j & 1]
    even = [j for j in range(parts) if not j & 1]
    total, routed_rows = {}, {}
    last_picked = last_act = last_left = last_weigh = ()
    for g, members in enumerate(groups):
        mine = [blocks[k] for k in members]
        picked, weight, taking = step(dispatch, *mine, after=last_picked)
        last_picked = (picked, weight, taking)

        slices = {0: picked}
        if g:
            picked_far = step(pick, taking, *[far[k] for k in members])
            for n, j in enumerate(others):
                slices[j] = picked_far[:, n * width : (n + 1) * width]
        else:
            for bit in part_bits[1:]:
                for j in list(slices):
                    slices[j | bit] = swap(slices[j], dm=bit)
        own = jnp.stack([slices[j] for j in even])
        core = swap(own, dm=1)

        held = step(lambda *b: tuple(by_part([x[:rows] for x in b])), *mine)

        def sums_of(js, kind):
            return lambda w, *h: dot(jnp.concatenate([h[j] for j in js]), w).astype(kind)

        leaving = step(sums_of(odd, BF16), both, *held)
        staying = step(sums_of(even, F32), both, *held)
        sums = {j: staying[i * rows : (i + 1) * rows] for i, j in enumerate(even)}
        pending = list(range(parts))
        for bit in part_bits:
            keep = [j for j in pending if not j & bit]
            if bit > 1:
                adds = [sums[j] for j in pending]

                def add(*v):
                    added = [x + y.astype(F32) for x, y in zip(v[::2], v[1::2])]
                    left = [x.astype(BF16) for x, j in zip(added, pending) if j & bit]
                    return jnp.concatenate(left), [x for x, j in zip(added, pending) if not j & bit]

                flat = [x for pair in adds for x in pair]
                leaving, stay = step(add, *flat, after=last_left)
                last_left = (leaving,)
                sums = dict(zip(keep, stay))
            came = swap(leaving, dm=bit)
            if 2 * bit == parts:
                break
            for i, j in enumerate(keep):
                sums[j] = (sums[j], came[i * rows : (i + 1) * rows])
            pending = keep
        act = step(shared_act, sums[0], came, after=last_act)
        last_act = (act,)

        known = {0: act}
        for bit in reversed(part_bits):
            order = sorted(known)
            got = swap(jnp.concatenate([known[j] for j in order]), dm=bit)
            for n, j in enumerate(order):
                known[j | bit] = got[n * rows : (n + 1) * rows]
        shared_hidden = step(lambda *v: tuple(by_part(v)), *[known[j] for j in range(parts)])

        hidden = step(feed, own, core)
        leaving = step(lower(odd, BF16), hidden)
        staying = step(lower(even, F32), hidden)
        partial = {j: staying[i] for i, j in enumerate(even)}
        pending = list(range(parts))
        for bit in part_bits:
            keep = [j for j in pending if not j & bit]
            if bit > 1:
                adds = [partial[j] for j in pending]

                def add_rows(*v):
                    added = [x + y.astype(F32) for x, y in zip(v[::2], v[1::2])]
                    left = [x.astype(BF16) for x, j in zip(added, pending) if j & bit]
                    return jnp.stack(left), [x for x, j in zip(added, pending) if not j & bit]

                flat = [x for pair in adds for x in pair]
                leaving, stay = step(add_rows, *flat, after=last_weigh)
                last_weigh = (leaving,)
                partial = dict(zip(keep, stay))
            came = swap(leaving, dm=bit)
            if 2 * bit < parts:
                for i, j in enumerate(keep):
                    partial[j] = (partial[j], came[i])
            pending = keep
        routed_rows[g] = (partial[0], came[0], weight, taking, shared_hidden)

    def weigh(result, came, weight):
        result = (result + came.astype(F32)).reshape(parts, slots, width)
        return (result * weight[:, :, None]).astype(BF16)

    def join(hidden, result, taking):
        routed = jnp.einsum("st,sd->td", taking, result, preferred_element_type=F32)
        return dot(hidden, shared_down_weight) + routed

    last_weigh = ()
    for g, members in reversed(list(enumerate(groups))):
        here, came, weight, taking, shared_hidden = routed_rows[g]
        result = step(weigh, here, came, weight, after=last_weigh)
        last_weigh = (result,)
        for i, k in enumerate(members):
            total[k] = join(shared_hidden[i], result[i], taking[i])

    left = list(range(experts))
    for bit in expert_bits:
        for k in sorted((k for k in left if k & bit), reverse=True):
            came = swap(total[k].astype(BF16), de=bit)
            total[k ^ bit] = total[k ^ bit] + came.astype(F32)
        left = [k for k in left if not k & bit]
    return total[0].astype(BF16)


def solution(mesh):
    in_specs = (
        P("expert", "mp"),
        P("expert", None),
        P("expert", None),
        P("expert", None, "mp"),
        P("expert", None, "mp"),
        P("expert", "mp", None),
        P("mp", "expert"),
        P("mp", "expert"),
        P("expert", "mp"),
    )
    out_specs = P("expert", "mp")
    return jax.shard_map(
        on_device, mesh=mesh, in_specs=in_specs, out_specs=out_specs, check_vma=False
    )
```

```python
import jax
import jax.numpy as jnp
from jax import lax
from jax.sharding import PartitionSpec as P


BF16 = jnp.bfloat16
F32 = jnp.float32


def bits_of(size):
    count = size.bit_length() - 1
    assert size == 1 << count
    return [1 << b for b in range(count)]


def dot(a, b):
    return jnp.dot(a, b, preferred_element_type=F32)


def three_parts(values):
    parts = []
    for _ in range(3):
        head = lax.reduce_precision(values, 8, 7)
        parts.append(head.astype(BF16))
        values = values - head
    return parts


def step(function, *values, after=()):
    held = lax.optimization_barrier(values + tuple(after))[: len(values)]
    return function(*held)


def on_device(
    tokens,
    assignments,
    gate_probs,
    expert_gate,
    expert_up,
    expert_down,
    shared_gate,
    shared_up,
    shared_down_weight,
):
    experts, parts = lax.axis_size("expert"), lax.axis_size("mp")
    expert, part = lax.axis_index("expert"), lax.axis_index("mp")
    rows, width = tokens.shape
    chosen = assignments.shape[1]
    slots = min(rows, max(2, 2 * rows * chosen // experts))
    expert_bits, part_bits = bits_of(experts), bits_of(parts)
    groups = [list(range(g, g + parts)) for g in range(0, experts, parts)]
    hidden_width = shared_gate.shape[1]

    flips = [(part & bit) != 0 for bit in part_bits]
    starts = [(part ^ j) * width for j in range(parts)]
    expert_number = expert.astype(F32)

    def swap(value, de=0, dm=0):
        pairs = [
            (e * parts + m, (e ^ de) * parts + (m ^ dm))
            for e in range(experts)
            for m in range(parts)
        ]
        return lax.ppermute(value, ("expert", "mp"), pairs)

    def by_part(values):
        values = list(values)
        for bit, flip in zip(part_bits, flips):
            values = [jnp.where(flip, values[j ^ bit], values[j]) for j in range(len(values))]
        return values

    def prepare(tokens, ids, probs):
        notes = [ids.T[k : k + 1].astype(BF16) for k in range(chosen)]
        for k in range(chosen):
            notes += three_parts(probs.T[k : k + 1])
        notes = jnp.concatenate(notes, axis=0)
        return jnp.concatenate([tokens, jnp.pad(notes, ((0, 0), (0, width - rows)))], axis=0)

    blocks = {0: step(prepare, tokens, assignments, gate_probs)}
    for bit in reversed(expert_bits[1:]):
        for k in list(blocks):
            blocks[k | bit] = swap(blocks[k], de=bit)
    for k in list(blocks):
        blocks[k | 1] = swap(blocks[k], de=1)

    slices = {0: tokens}
    for bit in part_bits[1:]:
        for j in list(slices):
            slices[j | bit] = swap(slices[j], dm=bit)
    others = [j for j in sorted(slices) if j]
    far = {0: jnp.concatenate([slices[j] for j in others], axis=1)}
    for bit in reversed(expert_bits):
        source = [k for k in sorted(far) if bit >= parts or k >= parts]
        if source:
            got = swap(jnp.stack([far[k] for k in source]), de=bit)
            for n, k in enumerate(source):
                far[k | bit] = got[n]

    before = jnp.triu(jnp.ones((rows, rows), F32), 1).astype(BF16)
    place = jnp.arange(slots, dtype=jnp.int32).astype(F32)[None, :, None]
    both = step(lambda a, b: jnp.concatenate([a, b], axis=1), shared_gate, shared_up)

    def pick(taking, *sources):
        return jnp.concatenate([dot(taking[i], b).astype(BF16) for i, b in enumerate(sources)])

    def dispatch(*members):
        table = jnp.stack([b[rows : rows + 4 * chosen, :rows] for b in members])
        ids = table[:, :chosen].astype(F32)
        probs = table[:, chosen:].astype(F32).reshape(len(members), chosen, 3, rows)
        probs = probs[:, :, 0] + (probs[:, :, 1] + probs[:, :, 2])
        mine = ids == expert_number
        named = jnp.any(mine, axis=1).astype(F32)
        rank = dot(named.astype(BF16), before)
        taking = ((rank[:, None, :] == place) & (named[:, None, :] > 0)).astype(BF16)
        row_prob = jnp.sum(jnp.where(mine, probs, 0.0), axis=1)
        return pick(taking, *[b[:rows] for b in members]), row_prob, taking

    def slot_weights(row_prob, taking):
        return jnp.sum(taking.astype(F32) * row_prob[:, None, :], axis=2)

    def shared_act(act, came):
        act = act + came.astype(F32)
        return (jax.nn.silu(act[:, :hidden_width]) * act[:, hidden_width:]).astype(BF16)

    def cut(weights, j, axis):
        at, sizes = [0, 0], list(weights.shape)
        at[axis], sizes[axis] = starts[j], width
        return lax.dynamic_slice(weights, at, sizes, allow_negative_indices=False)

    def feed(own, core):
        gate_act = up_act = 0.0
        for j in sorted(range(parts), key=lambda j: j & 1):
            rows_j = core[j // 2] if j & 1 else own[j // 2]
            gate_act += dot(rows_j, cut(expert_gate[0], j, 0))
            up_act += dot(rows_j, cut(expert_up[0], j, 0))
        return (jax.nn.silu(gate_act) * up_act).astype(BF16)

    def lower(js, kind):
        def function(hidden):
            out = []
            for j in js:
                out.append(dot(hidden, cut(expert_down[0], j, 1)).astype(kind))
            return jnp.stack(out)

        return function

    def halve(js, bit, height):
        def function(staying, came):
            go, keep = [], []
            for i, j in enumerate(js):
                span = slice(i * height, (i + 1) * height)
                value = staying[span] + came[span].astype(F32)
                (go if j & bit else keep).append(value)
            return jnp.concatenate([v.astype(BF16) for v in go]), jnp.concatenate(keep)

        return function

    odd = [j for j in range(parts) if j & 1]
    even = [j for j in range(parts) if not j & 1]
    total, routed_rows, returned, shared_hidden = {}, {}, {}, {}
    last_picked = last_act = last_left = last_weigh = ()
    for g, members in enumerate(groups):
        mine = [blocks[k] for k in members]
        routed_order = sorted(members, key=lambda k: (not k & 1, -k))
        picked, row_prob, taking = step(
            dispatch, *[blocks[k] for k in routed_order], after=last_picked
        )
        last_picked = (picked, row_prob, taking)
        weight = step(slot_weights, row_prob, taking)

        slices = {0: picked}
        if g:
            picked_far = step(pick, taking, *[far[k] for k in routed_order])
            for n, j in enumerate(others):
                slices[j] = picked_far[:, n * width : (n + 1) * width]
        else:
            for bit in part_bits[1:]:
                for j in list(slices):
                    slices[j | bit] = swap(slices[j], dm=bit)
        own = step(lambda *v: jnp.stack(v), *[slices[j] for j in even])
        core = swap(own, dm=1)

        held = step(lambda *b: tuple(by_part([x[:rows] for x in b])), *mine)

        def sums_of(js, kind):
            return lambda w, *h: dot(jnp.concatenate([h[j] for j in js]), w).astype(kind)

        leaving = step(sums_of(odd, BF16), both, *held)
        staying = step(sums_of(even, F32), both, *held)
        came = swap(leaving, dm=1)
        pending = even
        for bit in part_bits[1:]:
            leaving, staying = step(halve(pending, bit, rows), staying, came, after=last_left)
            last_left = (leaving,)
            came = swap(leaving, dm=bit)
            pending = [j for j in pending if not j & bit]
        act = step(shared_act, staying, came, after=last_act)
        last_act = (act,)

        arrays, known = [act], {0: (0, 0)}
        for bit in reversed(part_bits):
            order = sorted(known)
            got = swap(jnp.concatenate(arrays), dm=bit)
            flat = [j for i in range(len(arrays)) for j in order if known[j][0] == i]
            for n, j in enumerate(flat):
                known[j | bit] = (len(arrays), n)
            arrays.append(got)
        returned[g] = (arrays, known)

        hidden = step(feed, own, core)
        leaving = step(lower(odd, BF16), hidden)
        staying = step(lower(even, F32), hidden)
        came = swap(leaving, dm=1)
        spans = [("a", 0, 2), ("b", 1, 2)] if g == 0 else [("", 0, 1)]
        for tag, at, pieces in spans:
            height = parts * slots // pieces
            stay, got, pending = staying, came, even
            for bit in part_bits[1:]:

                def add_rows(stay, got):
                    first = height * at if stay.shape[1] > height else 0
                    span = slice(first, first + height)
                    added = [stay[i, span] + got[i, span].astype(F32) for i in range(len(pending))]
                    go = [x.astype(BF16) for x, j in zip(added, pending) if j & bit]
                    return jnp.stack(go), jnp.stack([x for x, j in zip(added, pending) if not j & bit])

                sent, stay = step(add_rows, stay, got, after=last_weigh)
                last_weigh = (sent,)
                got = swap(sent, dm=bit)
                pending = [j for j in pending if not j & bit]
            inside = slice(at * parts // pieces, (at + 1) * parts // pieces)
            order = routed_order[inside]
            routed_rows[f"{g}{tag}"] = (order, stay, got, weight, taking, inside)

    def weigh(result, came, weight):
        result = (result + came.astype(F32)).reshape(-1, slots, width)
        return (result * weight[inside][:, :, None]).astype(BF16)

    def join(hidden, result, taking):
        routed = jnp.einsum(
            "st,sd->td", taking[inside][i], result[i], preferred_element_type=F32
        )
        return dot(hidden, shared_down_weight) + routed

    last_weigh = ()
    for name in sorted(routed_rows, key=lambda n: (-int(n.rstrip("ab")), n)):
        order, here, came, weight, taking, inside = routed_rows[name]
        g = int(name.rstrip("ab"))
        if groups[g][0] not in shared_hidden:
            arrays, known = returned[g]

            def turn(*v):
                at = [known[j] for j in range(parts)]
                return tuple(by_part([v[i][n * rows : (n + 1) * rows] for i, n in at]))

            back = step(turn, *arrays, after=last_weigh)
            shared_hidden.update(zip(groups[g], back))
            last_weigh = (back[0],)
        result = step(weigh, here, came, weight, after=last_weigh)
        last_weigh = (result,)
        for i, k in enumerate(order):
            total[k] = step(join, shared_hidden[k], result, taking)

    left = list(range(experts))
    for bit in expert_bits:
        for k in sorted((k for k in left if k & bit), reverse=True):
            leaving = total[k].astype(BF16)
            came = swap(leaving, de=bit)
            total[k ^ bit] = total[k ^ bit] + came.astype(F32)
        left = [k for k in left if not k & bit]
    return total[0].astype(BF16)


def solution(mesh):
    in_specs = (
        P("expert", "mp"),
        P("expert", None),
        P("expert", None),
        P("expert", None, "mp"),
        P("expert", None, "mp"),
        P("expert", "mp", None),
        P("mp", "expert"),
        P("mp", "expert"),
        P("expert", "mp"),
    )
    out_specs = P("expert", "mp")
    return jax.shard_map(
        on_device, mesh=mesh, in_specs=in_specs, out_specs=out_specs, check_vma=False
    )
```
